32 devices in a mesh: dp: 8 (over z, y), tp: 4 (over x, core).
Axes of the slice: x: 2, y: 2, z: 4, core: 2. Of those that a mesh axis runs over, the one named last changes fastest.
Arguments:
- queries: bfloat16 [2048, 4096], P('dp', 'tp'), may hold values from -6 to 6
- keys: bfloat16 [2048, 512], P(('dp', 'tp')), may hold values from -6 to 6
- values: bfloat16 [2048, 512], P(('dp', 'tp')), may hold values from -6 to 6
- out_weight: bfloat16 [4096, 8192], P('tp', 'dp'), may hold values from -0.09375 to 0.09375
- residual: bfloat16 [2048, 8192], P(('dp', 'tp')), may hold values from -40 to 40
- norm_gain: float32 [8192], replicated, may hold values from 0.5 to 1.5
Outputs:
- hidden_out: bfloat16 [2048, 8192], P(('dp', 'tp'))
- normed: bfloat16 [2048, 8192], P(('dp', 'tp'))
The draws below stay inside these ranges and needn't reach their ends.
All inputs are finite; a program needn't handle non-finite values.
Results may differ from the reference program's by a relative error of at most 0.012.
Values may be sent and summed in bfloat16 or wider, within the bound.
No kernel may reach another device: no remote copies, remote signals or barrier semaphores. Data moves between devices by JAX's collectives and lax.ppermute only.
A program may use at most 64 MiB of HBM per device.

```python
import math
import jax
import jax.numpy as jnp
from jax import lax

D = 8192
HQ = 32
KVH = 4
HDIM = 128
LEN = 32
TOKENS = 2048
N_TP = 4


def draw_queries(key, part):
    base = jax.random.truncated_normal(jax.random.fold_in(key, 1), -6.0, 6.0, (TOKENS, HQ * HDIM), jnp.float32)
    return base.astype(jnp.bfloat16)


def draw_keys(key, part):
    base = jax.random.truncated_normal(jax.random.fold_in(key, 2), -6.0, 6.0, (TOKENS, KVH * HDIM), jnp.float32)
    return base.astype(jnp.bfloat16)


def draw_residual(key, part):
    base = jax.random.truncated_normal(jax.random.fold_in(key, 3), -6.0, 6.0, (TOKENS, D), jnp.float32)
    lowest = 0.08
    row_scale = jnp.exp(jax.random.uniform(jax.random.fold_in(key, 4), (TOKENS, 1), jnp.float32, math.log(lowest), math.log(10.0 * lowest)))
    column_scale = jnp.exp(jax.random.uniform(jax.random.fold_in(key, 5), (1, D), jnp.float32, math.log(0.35), math.log(3.5)))
    return jnp.clip(base * row_scale * column_scale, -40.0, 40.0).astype(jnp.bfloat16)


def level_of(rng, dims, shards, least, largest):
    loudness = 1.0
    for axis_at, blocks in shards:
        heights = jax.random.uniform(jax.random.fold_in(jax.random.fold_in(rng, 6), axis_at), (blocks,), jnp.float32, least / len(shards), largest / len(shards))
        loudness = loudness * jnp.repeat(jnp.exp(heights), dims[axis_at] // blocks).reshape((-1,) + (1,) * (len(dims) - 1 - axis_at))
    return loudness


def noise(rng, shape, scale, reach, cuts=(), held_as=jnp.bfloat16):
    factor_of = level_of(rng, shape, cuts, -0.22, 0.18) if cuts else 1.0
    result = jax.random.normal(rng, shape, jnp.float32) * scale * factor_of
    return jnp.minimum(jnp.maximum(result, -reach), reach).astype(held_as)


def setup_inputs(seed: int = 0) -> dict:
    key_of = jax.random.split(jax.random.key(seed), 7)
    return {
        "queries": draw_queries(jax.random.fold_in(key_of[6], 71), 0),
        "keys": draw_keys(jax.random.fold_in(key_of[6], 71), 0),
        "values": noise(key_of[2], (TOKENS, KVH * HDIM), 1.0, 6.0, ((0, 32),)),
        "out_weight": noise(key_of[3], (HQ * HDIM, D), (HQ * HDIM) ** -0.5, 0.09375, ((0, 4), (1, 8))),
        "residual": draw_residual(jax.random.fold_in(key_of[6], 71), 0),
        "norm_gain": jnp.clip(1.0 + 0.1 * jax.random.normal(key_of[5], (D,), jnp.float32), 0.5, 1.5),
    }


def attend(queries, keys, values):
    sequences = queries.shape[0] // LEN
    group = HQ // KVH
    query_heads = queries.reshape(sequences, LEN, HQ, HDIM).astype(jnp.float32)
    key_heads = jnp.repeat(keys.reshape(sequences, LEN, KVH, HDIM).astype(jnp.float32), group, axis=2)
    value_heads = jnp.repeat(values.reshape(sequences, LEN, KVH, HDIM).astype(jnp.float32), group, axis=2)
    scores = jnp.einsum('slhd,smhd->shlm', query_heads, key_heads) / math.sqrt(HDIM)
    causal = jnp.arange(LEN)[:, None] >= jnp.arange(LEN)[None, :]
    scores = jnp.where(causal, scores, -1e+30)
    highest = lax.optimization_barrier(jnp.max(scores, axis=-1, keepdims=True))
    powers = jnp.exp(scores - highest)
    weights = (powers / lax.optimization_barrier(jnp.sum(powers, axis=-1, keepdims=True))).astype(jnp.bfloat16)
    attended = jnp.einsum('shlm,smhd->slhd', weights.astype(jnp.float32), value_heads)
    return attended.astype(jnp.bfloat16).reshape(queries.shape[0], HQ * HDIM)

def reference(queries, keys, values, out_weight, residual, norm_gain):
    attended = attend(queries, keys, values)
    width = HQ * HDIM // N_TP
    projected = jnp.zeros((queries.shape[0], D), jnp.float32)
    for block in range(N_TP):
        term = jnp.dot(attended[:, block * width:(block + 1) * width], out_weight[block * width:(block + 1) * width], preferred_element_type=jnp.float32)
        rounded = lax.optimization_barrier(term.astype(jnp.bfloat16))
        projected = projected + rounded.astype(jnp.float32)
    updated = residual.astype(jnp.float32) + projected
    hidden_out = updated.astype(jnp.bfloat16)
    meansq = lax.optimization_barrier(jnp.mean(updated * updated, axis=-1, keepdims=True))
    normed = (updated * lax.rsqrt(meansq + 1e-05) * norm_gain).astype(jnp.bfloat16)
    return (hidden_out, normed)
```

```python
import math

import jax
import jax.numpy as jnp
from jax import lax
from jax.experimental import pallas as pl
from jax.experimental.pallas import tpu as pltpu
from jax.sharding import PartitionSpec as P

KVH = 4
HDIM = 128
LEN = 32
STEPS = 4


def attention(queries, key_head, value_head):
    rows = queries.shape[0]
    sequences = rows // LEN
    local_heads = queries.shape[1] // HDIM
    query_heads = queries.reshape(sequences, LEN, local_heads, HDIM)
    key_rows = key_head.reshape(sequences, LEN, HDIM)
    value_rows = value_head.reshape(sequences, LEN, HDIM)
    scores = jnp.einsum(
        "slhd,smd->shlm", query_heads, key_rows, preferred_element_type=jnp.float32
    ) / math.sqrt(HDIM)
    causal = jnp.arange(LEN)[:, None] >= jnp.arange(LEN)[None, :]
    scores = jnp.where(causal, scores, -1e30)
    highest = jnp.max(scores, axis=-1, keepdims=True)
    powers = jnp.exp(scores - highest)
    weights = (powers / jnp.sum(powers, axis=-1, keepdims=True)).astype(jnp.bfloat16)
    attended = jnp.einsum("shlm,smd->slhd", weights, value_rows, preferred_element_type=jnp.float32)
    return attended.astype(jnp.bfloat16).reshape(rows, local_heads * HDIM)


def finish(width, n_groups, columns_ref, residual_ref, gain_ref, *refs):
    pieces, (hidden_ref, normed_ref, updated_ref) = refs[:-3], refs[-3:]
    total = jnp.zeros((residual_ref.shape[0], 1), jnp.float32)
    slot = 0
    for piece in pieces:
        for start in range(0, piece.shape[1], width):
            at = pl.ds(pl.multiple_of(columns_ref[slot] * width, width), width)
            block = piece[:, start : start + width].astype(jnp.float32)
            updated = residual_ref[:, at].astype(jnp.float32) + block
            updated_ref[:, at] = updated
            hidden_ref[:, at] = updated.astype(jnp.bfloat16)
            total += jnp.sum(updated * updated, axis=-1, keepdims=True)
            slot += 1
    scale = lax.rsqrt(total / residual_ref.shape[1] + 1e-05)
    for slot in range(n_groups):
        at = pl.ds(slot * width, width)
        normed_ref[:, at] = (updated_ref[:, at] * scale * gain_ref[:, at]).astype(jnp.bfloat16)


def local(queries, keys, values, out_weight, residual, norm_gain):
    tp_size, dp_size = lax.axis_size("tp"), lax.axis_size("dp")
    tp_at, dp_at = lax.axis_index("tp"), lax.axis_index("dp")
    n_outer, n_far = math.gcd(dp_size, STEPS), tp_size // 2
    n_inner = dp_size // n_outer
    outer, inner = dp_at // n_inner, dp_at % n_inner
    far, near = tp_at // 2, tp_at % 2
    rows, width = keys.shape[0], out_weight.shape[1]

    def over_dp(value, steps, inner_steps=0):
        pairs = [
            (
                o * n_inner + i,
                (o + steps) % n_outer * n_inner + (i + inner_steps) % n_inner,
            )
            for o in range(n_outer)
            for i in range(n_inner)
        ]
        return lax.ppermute(value, "dp", pairs)

    def over_tp(value, steps, flip=0):
        pairs = [
            (q * 2 + c, (q + steps) % n_far * 2 + (c ^ flip))
            for q in range(n_far)
            for c in range(2)
        ]
        return lax.ppermute(value, "tp", pairs)

    others = [over_dp(out_weight, 0, -k) for k in range(1, n_inner)]
    weights = [out_weight, jnp.concatenate(others, axis=1)]
    shifts = [[0], list(range(1, n_inner))]

    heads = jnp.stack(
        [
            jnp.concatenate(
                [part[:, h * HDIM : (h + 1) * HDIM] for part in (keys, values)], axis=1
            )
            for h in (j * KVH // tp_size for j in range(tp_size))
        ]
    )
    heads = lax.all_to_all(heads, "tp", 0, 0).reshape(tp_size * rows, 2 * HDIM)
    attended = attention(queries, heads[:, :HDIM], heads[:, HDIM:])
    depth = attended.shape[1]

    blocks = attended.reshape(n_far, 2, rows, depth)
    order = [
        lax.dynamic_index_in_dim(
            lax.dynamic_index_in_dim(blocks, (far + k) % n_far, 0, False), c, 0, False
        )
        for c in (1 - near, near)
        for k in range(n_far)
    ]
    chunk = jnp.concatenate(order, axis=0)
    half = rows * n_far

    landed = [[None] * n_outer for _ in range(2)]
    for step in range(n_outer):
        following = over_dp(chunk, 1) if step < n_outer - 1 else None
        for side in range(2):
            partial = jnp.dot(chunk, weights[side], preferred_element_type=jnp.float32)
            sent = over_tp(partial[:half].astype(jnp.bfloat16), 0, 1)
            total = partial[half:] + sent.astype(jnp.float32)
            mine = total[:rows]
            for k in range(1, n_far):
                part = total[k * rows : (k + 1) * rows].astype(jnp.bfloat16)
                mine += over_tp(part, k).astype(jnp.float32)
            mine = mine.astype(jnp.bfloat16)
            landed[side][step] = over_dp(mine, -step) if step else mine
        chunk = following

    columns = jnp.stack(
        [
            (outer + step) % n_outer * n_inner + (inner + k) % n_inner
            for side in range(2)
            for step in range(n_outer)
            for k in shifts[side]
        ]
    ).astype(jnp.int32)
    shape = jax.ShapeDtypeStruct(residual.shape, jnp.bfloat16)
    vmem = pl.BlockSpec(memory_space=pltpu.VMEM)
    return pl.pallas_call(
        lambda *refs: finish(width, dp_size, *refs),
        out_shape=(shape, shape),
        in_specs=[pl.BlockSpec(memory_space=pltpu.SMEM)] + [vmem] * (2 + 2 * n_outer),
        out_specs=(vmem, vmem),
        scratch_shapes=[pltpu.VMEM(residual.shape, jnp.float32)],
        name="finish",
    )(columns, residual, norm_gain.reshape(1, -1), *landed[0], *landed[1])


def solution(mesh):
    return jax.shard_map(
        local,
        mesh=mesh,
        in_specs=(
            P("dp", "tp"),
            P(("dp", "tp"), None),
            P(("dp", "tp"), None),
            P("tp", "dp"),
            P(("dp", "tp"), None),
            P(),
        ),
        out_specs=(P(("dp", "tp"), None), P(("dp", "tp"), None)),
        check_vma=False,
    )
```

```python
import functools
import math

import jax
import jax.numpy as jnp
from jax import lax
from jax.experimental import pallas as pl
from jax.experimental.pallas import tpu as pltpu
from jax.sharding import PartitionSpec as P


KVH = 4
HDIM = 128
LEN = 32
STEPS = 4
VMEM = pl.BlockSpec(memory_space=pltpu.VMEM)
PARAMS = pltpu.CompilerParams(vmem_limit_bytes=16 * 1024 * 1024)


def tp_place():
    at = lax.axis_index("tp")
    return at // 2, at % 2, lax.axis_size("tp") // 2


def turns(n_far):
    return [(k, flip) for k in range(n_far) for flip in ((0, 1) if k == 0 else (1, 0))]


def share(keys_ref, values_ref, *block_refs):
    far, near, n_far = tp_place()
    for (k, flip), block_ref in zip(turns(n_far), block_refs):
        target = (far + k) % n_far * 2 + (near + flip) % 2
        head = target * KVH // (2 * n_far)
        lanes = pl.ds(pl.multiple_of(head * HDIM, HDIM), HDIM)
        block_ref[:, :HDIM] = keys_ref[:, lanes]
        block_ref[:, HDIM:] = values_ref[:, lanes]


def gather(*refs):
    *block_refs, held_ref = refs
    far, near, n_far = tp_place()
    rows = block_refs[0].shape[0]
    for (k, flip), block_ref in zip(turns(n_far), block_refs):
        source = (far + n_far - k) % n_far * 2 + (near + flip) % 2
        held_ref[pl.ds(pl.multiple_of(source * rows, rows), rows), :] = block_ref[...]


def attend(rows, queries_ref, held_ref, out_ref):
    far, near, n_far = tp_place()
    tokens = held_ref.shape[0]
    group = min(tokens, 4 * LEN)
    heads = queries_ref.shape[1] // HDIM
    at_query = lax.broadcasted_iota(jnp.int32, (group, group), 0)
    at_key = lax.broadcasted_iota(jnp.int32, (group, group), 1)
    seen = (at_query // LEN == at_key // LEN) & (at_query >= at_key)
    for first in range(0, tokens, group):
        queries = jnp.concatenate(
            [queries_ref[first : first + group, h * HDIM : (h + 1) * HDIM] for h in range(heads)],
            axis=0,
        )
        scores = lax.dot_general(
            queries,
            held_ref[first : first + group, :HDIM],
            (((1,), (1,)), ((), ())),
            preferred_element_type=jnp.float32,
        ) * (1 / math.sqrt(HDIM))
        scores = jnp.where(seen[None], scores.reshape(heads, group, group), -1e30)
        powers = jnp.exp(scores - jnp.max(scores, axis=-1, keepdims=True))
        powers = powers.astype(jnp.bfloat16).reshape(heads * group, group)
        values = jnp.concatenate(
            [held_ref[first : first + group, HDIM:], jnp.ones((group, HDIM), jnp.bfloat16)], axis=1
        )
        attended = jnp.dot(powers, values, preferred_element_type=jnp.float32)
        attended = (attended[:, :HDIM] / attended[:, HDIM:]).astype(jnp.bfloat16)
        for start in range(0, group, rows):
            device = (first + start) // rows
            place = (device // 2 + n_far - far) % n_far + (near + device + 1) % 2 * n_far
            at = pl.ds(pl.multiple_of(place * rows, rows), rows)
            for head in range(heads):
                block = head * group + start
                out_ref[at, head * HDIM : (head + 1) * HDIM] = attended[block : block + rows]


def project(products, n_chunks, *refs):
    *sources, sent_ref, kept_ref = refs
    chunks, pieces = sources[:n_chunks], sources[n_chunks:]
    half, start = sent_ref.shape[0], 0
    for chunk, piece in products:
        width = pieces[piece].shape[1]
        step = math.gcd(width, 512)
        for at in range(0, width, step):
            total = jnp.dot(
                chunks[chunk][...],
                pieces[piece][:, at : at + step],
                preferred_element_type=jnp.float32,
            )
            lanes = slice(start + at, start + at + step)
            sent_ref[:, lanes] = total[:half].astype(jnp.bfloat16)
            kept_ref[:, lanes] = total[half:]
        start += width


def finish(n_inner, unit, slots, residual_ref, gain_ref, *refs):
    pieces = refs[: len(slots)]
    hidden_ref, normed_ref, updated_ref = refs[len(slots) :]
    at = lax.axis_index("dp")
    outer, inner = at // n_inner, at % n_inner
    split = residual_ref.shape[1] // (unit * lax.axis_size("dp"))
    total = jnp.zeros((residual_ref.shape[0], 1), jnp.float32)
    for piece, owned in zip(pieces, slots):
        for place, (j, k, part) in enumerate(owned):
            column = ((outer ^ j) * n_inner + (inner + k) % n_inner) * split + part
            at = pl.ds(pl.multiple_of(column * unit, unit), unit)
            block = piece[:, place * unit : (place + 1) * unit].astype(jnp.float32)
            updated = residual_ref[:, at].astype(jnp.float32) + block
            updated_ref[:, at] = updated
            hidden_ref[:, at] = updated.astype(jnp.bfloat16)
            total += jnp.sum(updated * updated, axis=-1, keepdims=True)
    scale = lax.rsqrt(total / residual_ref.shape[1] + 1e-05)
    for slot in range(residual_ref.shape[1] // unit):
        at = pl.ds(slot * unit, unit)
        normed_ref[:, at] = (updated_ref[:, at] * scale * gain_ref[:, at]).astype(jnp.bfloat16)


def local(queries, keys, values, out_weight, residual, norm_gain):
    tp_size, dp_size = lax.axis_size("tp"), lax.axis_size("dp")
    n_outer, n_far = math.gcd(dp_size, STEPS), tp_size // 2
    n_inner = dp_size // n_outer
    rows, width = keys.shape[0], out_weight.shape[1]
    split = 2 if n_inner == 2 else 1
    unit = width // split

    def over_inner(value, steps):
        pairs = [
            (o * n_inner + i, o * n_inner + (i + steps) % n_inner)
            for o in range(n_outer)
            for i in range(n_inner)
        ]
        return lax.ppermute(value, "dp", pairs)

    def over_outer(value, pairs):
        every = [(a * n_inner + i, b * n_inner + i) for a, b in pairs for i in range(n_inner)]
        return lax.ppermute(value, "dp", every)

    def crossed(j):
        return [(o, o ^ j) for o in range(n_outer)]

    def over_tp(value, steps, flip):
        pairs = [
            (q * 2 + c, (q + steps) % n_far * 2 + (c ^ flip))
            for q in range(n_far)
            for c in range(2)
        ]
        return lax.ppermute(value, "tp", pairs)

    if n_inner == 2:
        units = [[(0, h) for h in range(split)], [(1, 0)], [(1, 1)]]
    else:
        middle = n_inner // 2 + 1
        units = [[(0, 0)], [(k, 0) for k in range(1, middle)], [(k, 0) for k in range(middle, n_inner)]]
    block_type = jax.ShapeDtypeStruct((rows, 2 * HDIM), jnp.bfloat16)
    blocks = pl.pallas_call(
        share,
        out_shape=[block_type] * tp_size,
        in_specs=[VMEM, VMEM],
        out_specs=[VMEM] * tp_size,
        compiler_params=PARAMS,
        name="share",
    )(keys, values)
    later = lax.optimization_barrier((out_weight, blocks[0]))[0]
    if n_inner == 2:
        weights = [out_weight, over_inner(out_weight[:, :unit], 1), over_inner(later[:, unit:], 1)]
    else:
        weights = [out_weight] + [
            jnp.concatenate([over_inner(out_weight, -k) for k, _ in units[at]], axis=1)
            for at in (1, 2)
        ]
    blocks = [
        over_tp(block, k, flip) if k or flip else block
        for (k, flip), block in zip(turns(n_far), blocks)
    ]
    tokens, depth = queries.shape
    chunk_type = jax.ShapeDtypeStruct((tokens, depth), jnp.bfloat16)
    held = pl.pallas_call(
        gather,
        out_shape=jax.ShapeDtypeStruct((tokens, 2 * HDIM), jnp.bfloat16),
        in_specs=[VMEM] * len(blocks),
        out_specs=VMEM,
        compiler_params=PARAMS,
        name="gather",
    )(*blocks)
    own = pl.pallas_call(
        functools.partial(attend, rows),
        out_shape=chunk_type,
        in_specs=[VMEM, VMEM],
        out_specs=VMEM,
        cost_estimate=pl.CostEstimate(
            flops=4 * tokens * depth * 4 * LEN, bytes_accessed=4 * tokens * depth, transcendentals=0
        ),
        compiler_params=PARAMS,
        name="attend",
    )(queries, held)

    chunks = [own]
    if n_outer >= 2:
        chunks.append(over_outer(own, crossed(1)))
    if n_outer == 4:
        chunks.append(over_outer(own, crossed(2)))
        direct = over_outer(own, [(1, 2), (2, 1)])
        relayed = over_outer(chunks[2], [(1, 0), (2, 3)])
        chunks.append(direct + relayed)

    if n_outer == 4:
        events = [
            [(0, 0)],
            [(0, 1), (1, 0), (1, 1)],
            [(2, 0), (2, 1)],
            [(3, 0), (3, 1)],
            [(0, 2), (1, 2), (2, 2), (3, 2)],
        ]
    else:
        events = [[(j, piece) for j in range(n_outer) for piece in range(3)]]

    half = rows * n_far
    landed, slots = [], []
    for products in events:
        used = sorted({j for j, _ in products})
        held = sorted({piece for _, piece in products})
        total_width = sum(weights[piece].shape[1] for _, piece in products)
        sent, kept = pl.pallas_call(
            functools.partial(
                project, [(used.index(j), held.index(p)) for j, p in products], len(used)
            ),
            out_shape=(
                jax.ShapeDtypeStruct((half, total_width), jnp.bfloat16),
                jax.ShapeDtypeStruct((half, total_width), jnp.float32),
            ),
            in_specs=[VMEM] * (len(used) + len(held)),
            out_specs=(VMEM, VMEM),
            cost_estimate=pl.CostEstimate(
                flops=2 * tokens * depth * total_width,
                bytes_accessed=2 * depth * total_width,
                transcendentals=0,
            ),
            compiler_params=PARAMS,
        )(*[chunks[j] for j in used], *[weights[p] for p in held])
        total = kept + over_tp(sent, 0, 1).astype(jnp.float32)
        arrived = [
            over_tp(total[k * rows : (k + 1) * rows].astype(jnp.bfloat16), k, 0)
            for k in range(1, n_far)
        ]
        start = 0
        for j in used:
            pieces = [p for i, p in products if i == j]
            stop = start + sum(weights[p].shape[1] for p in pieces)
            mine = total[:rows, start:stop]
            for other in arrived:
                mine += other[:, start:stop].astype(jnp.float32)
            mine = mine.astype(jnp.bfloat16)
            landed.append(over_outer(mine, crossed(j)) if j else mine)
            slots.append([(j, k, part) for p in pieces for k, part in units[p]])
            start = stop

    shape = jax.ShapeDtypeStruct(residual.shape, jnp.bfloat16)
    return pl.pallas_call(
        functools.partial(finish, n_inner, unit, slots),
        out_shape=(shape, shape),
        in_specs=[VMEM] * (2 + len(landed)),
        out_specs=(VMEM, VMEM),
        scratch_shapes=[pltpu.VMEM(residual.shape, jnp.float32)],
        compiler_params=PARAMS,
        name="finish",
    )(residual, norm_gain.reshape(1, -1), *landed)


def solution(mesh):
    return jax.shard_map(
        local,
        mesh=mesh,
        in_specs=(
            P("dp", "tp"),
            P(("dp", "tp"), None),
            P(("dp", "tp"), None),
            P("tp", "dp"),
            P(("dp", "tp"), None),
            P(),
        ),
        out_specs=(P(("dp", "tp"), None), P(("dp", "tp"), None)),
        check_vma=False,
    )
```
